32 devices in a mesh: cosmo: 2 (over x), row: 16 (over z, y, core).
Axes of the slice: x: 2, y: 2, z: 4, core: 2. Of those that a mesh axis runs over, the one named last changes fastest.
Arguments:
- potentials: float32 [4, 256, 16384], P('cosmo', 'row'), parts along dimension 0, may hold values from -3 to 3
- ratios: float32 [6], P('cosmo'), parts along dimension 0, may hold values from 0.3 to 0.9
- row_offset: int32 [256], P('cosmo'), parts along dimension 0, may hold values from 0 to 7
- col_offset: int32 [256], P('cosmo'), parts along dimension 0, may hold values from 0 to 127
Outputs:
- convergence: float32 [512, 16384], P(('cosmo', 'row')), parts along dimension 0
- shear_map: float32 [2, 512, 16384], P(None, ('cosmo', 'row')), parts along dimension 1
- rotation: float32 [512, 16384], P(('cosmo', 'row')), parts along dimension 0
- displacement: float32 [2, 512, 16384], P(None, ('cosmo', 'row')), parts along dimension 1
The draws below stay inside these ranges and needn't reach their ends.
There are 2 independent parts, one for each index of `cosmo`. The reference program is written for one: setup_inputs(seed, part) draws one part's arguments, and reference() takes and returns one part's arrays. A program takes and returns all parts, laid end to end along the dimension named above; each array names one. Nothing has to cross between parts.
Inputs may be any that keep to these rules, and one draw needn't show every extreme that they name: `row_offset`: row offsets count blocks of 32 rows.
All inputs are finite; a program needn't handle non-finite values.
Results may differ from the reference program's by a relative error of at most 0.00002.
Values sent between devices are 32-bit elements; how exact they have to be, the bound alone decides.
A program may use at most 128 MiB of HBM per device.

```python
import jax
import jax.numpy as jnp

NC = 16384
PLANES = 2
RB = 8
NR = 256
NCB = 128


def plant(entries, own_key, smallest, high):
    spot = [jax.random.randint(jax.random.fold_in(own_key, axis), (), 0, length) for axis, length in enumerate(entries.shape)]
    main_axis = entries.shape.index(max(entries.shape))
    neighbour = spot[:main_axis] + [(spot[main_axis] + 1) % entries.shape[main_axis]] + spot[main_axis + 1:]
    return entries.at[tuple(spot)].set(smallest).at[tuple(neighbour)].set(high)


def level_of(key, dims, split, smallest, largest):
    level = 1.0
    for position, shards_of in split:
        draws = jax.random.uniform(jax.random.fold_in(jax.random.fold_in(key, 6), position), (shards_of,), jnp.float32, smallest / len(split), largest / len(split))
        level = level * jnp.repeat(jnp.exp(draws), dims[position] // shards_of).reshape((-1,) + (1,) * (len(dims) - 1 - position))
    return level


def centred(own_key, shape, spread, reach, cuts=(), kind=jnp.bfloat16):
    values = jax.random.normal(own_key, shape, jnp.float32) * spread
    if len(cuts) > 0:
        values = level_of(own_key, shape, cuts, -0.22, 0.18) * values
    return jnp.clip(values, min=-reach, max=reach).astype(kind)


def setup_inputs(seed: int = 0, part: int = 0) -> dict:
    splits = jax.random.split(jax.random.key(seed), 5)
    part_keys = jax.random.split(jax.random.fold_in(splits[4], part), 5)
    potentials = centred(part_keys[0], (PLANES, NR, NC), 0.5, 3.0, ((1, 16),), jnp.float32)
    ratios = jnp.clip(jax.random.uniform(part_keys[1], (3,), jnp.float32, 0.3, 0.9), 0.3, 0.9)
    row_offset = plant(jax.random.randint(part_keys[2], (NCB,), 0, RB), jax.random.fold_in(part_keys[2], 1), 0, RB - 1).astype(jnp.int32)
    col_offset = plant(jax.random.randint(part_keys[3], (NCB,), 0, NCB), jax.random.fold_in(part_keys[3], 1), 0, NCB - 1).astype(jnp.int32)
    return {"potentials": potentials, "ratios": ratios, "row_offset": row_offset, "col_offset": col_offset}


def slope_along(field, direction):
    return (8.0 * (jnp.roll(field, -1, direction) - jnp.roll(field, 1, direction)) - (jnp.roll(field, -2, direction) - jnp.roll(field, 2, direction))) / 12.0


def derive_plane(potential):
    slope_r = slope_along(potential, 0)
    slope_c = slope_along(potential, 1)
    return (slope_r, slope_c, slope_along(slope_r, 0), slope_along(slope_r, 1), slope_along(slope_c, 1))


def assemble(nearer, farther, ratios):
    near_r, near_c, near_rr, near_rc, near_cc = nearer
    far_r, far_c, far_rr, far_rc, far_cc = farther
    beta_near = ratios[0]
    beta_one = ratios[1]
    beta_two = ratios[2]
    inner_rr = 1.0 - beta_near * near_rr
    inner_rc = -beta_near * near_rc
    inner_cc = 1.0 - beta_near * near_cc
    chain_rr = far_rr * inner_rr + far_rc * inner_rc
    chain_rc = far_rr * inner_rc + far_rc * inner_cc
    chain_cr = far_rc * inner_rr + far_cc * inner_rc
    chain_cc = far_rc * inner_rc + far_cc * inner_cc
    total_rr = 1.0 - beta_one * near_rr - beta_two * chain_rr
    total_rc = -beta_one * near_rc - beta_two * chain_rc
    total_cr = -beta_one * near_rc - beta_two * chain_cr
    total_cc = 1.0 - beta_one * near_cc - beta_two * chain_cc
    convergence = 1.0 - 0.5 * (total_rr + total_cc)
    shear_map = jnp.stack([0.5 * (total_rr - total_cc), -0.5 * (total_rc + total_cr)])
    rotation = 0.5 * (total_rc - total_cr)
    displacement = jnp.stack([beta_one * near_r + beta_two * far_r, beta_one * near_c + beta_two * far_c])
    return convergence, shear_map, rotation, displacement


def reference(potentials, ratios, row_offset, col_offset):
    nearer = derive_plane(potentials[0])
    derived = derive_plane(potentials[1])
    blocks = NC // 128
    source = (jnp.arange(blocks, dtype=jnp.int32) + col_offset.astype(jnp.int32)) % blocks
    lookup_rows = (jnp.arange(NR, dtype=jnp.int32)[:, None] + (NR // RB) * row_offset.astype(jnp.int32)[None, :]) % NR

    def sample(field):
        strips = field.reshape(NR, blocks, 128)
        return strips[lookup_rows, source[None, :], :].reshape(NR, NC)

    farther = tuple(sample(member) for member in derived)
    return assemble(nearer, farther, ratios)
```

```python
import functools

import jax
import jax.numpy as jnp
from jax import lax
from jax.experimental import pallas as pl
from jax.experimental.pallas import tpu as pltpu
from jax.sharding import PartitionSpec as P

RB = 8
BITS = 3
LANES = 128
HALO = 4
PER_EDGE = LANES // (2 * HALO)
SPARE = 12
TILE = 16


def passed_along(x, axis, by):
    size = lax.axis_size(axis)
    return lax.ppermute(x, axis, [(i, (i + by) % size) for i in range(size)])


def edge_of(left, right, lane):
    return jnp.where(lane < LANES // 2, right, left)


def pack_kernel(cap, blocks, src_ref, pot_ref, out_ref):
    group = pl.program_id(0)
    rows = pot_ref.shape[1]
    lane = lax.broadcasted_iota(jnp.int32, (rows, LANES), 1)

    def at(s):
        return pot_ref[0, :, pl.ds(pl.multiple_of(s * LANES, LANES), LANES)]

    packed = None
    for j in range(cap):
        s = src_ref[group * cap + j]
        left = at(jnp.where(s == 0, blocks - 1, s - 1))
        right = at(jnp.where(s == blocks - 1, 0, s + 1))
        out_ref[0, j] = at(s)
        spot = j % PER_EDGE
        edge = pltpu.roll(edge_of(left, right, lane), HALO + 2 * HALO * spot, 1)
        packed = edge if spot == 0 else jnp.where(lane >= 2 * HALO * spot, edge, packed)
        if spot == PER_EDGE - 1 or j == cap - 1:
            out_ref[0, cap + j // PER_EDGE] = packed


def exchange_kernel(stride, devices, buf_ref, out_ref, send_sem, recv_sem, own_sem):
    me = lax.axis_index("row")
    barrier = pltpu.get_barrier_semaphore()
    for k in range(1, RB):
        pl.semaphore_signal(
            barrier,
            inc=1,
            device_id={"row": lax.rem(me + stride * k, devices)},
            device_id_type=pl.DeviceIdType.MESH,
        )
    pl.semaphore_wait(barrier, RB - 1)
    copies = []
    for k in range(1, RB):
        copy = pltpu.make_async_remote_copy(
            src_ref=buf_ref.at[k],
            dst_ref=out_ref.at[k],
            send_sem=send_sem.at[k],
            recv_sem=recv_sem.at[k],
            device_id={"row": lax.rem(me + devices - stride * k, devices)},
            device_id_type=pl.DeviceIdType.MESH,
        )
        copy.start()
        copies.append(copy)
    own = pltpu.make_async_copy(buf_ref.at[0], out_ref.at[0], own_sem)
    own.start()
    own.wait()
    for copy in copies:
        copy.wait()


def shifted(middle, edge, lane, by):
    if by > 0:
        return pltpu.roll(jnp.where(lane < by, edge, middle), LANES - by, 1)
    return pltpu.roll(jnp.where(lane >= LANES + by, edge, middle), -by, 1)


def second(x, total):
    return (
        (x[4] + x[-4]) - 16.0 * (x[3] + x[-3]) + 64.0 * (x[2] + x[-2])
        + 16.0 * (x[1] + x[-1]) - 130.0 * total
    ) * (1.0 / 144.0)


def first(x):
    return (8.0 * (x[1] - x[-1]) - (x[2] - x[-2])) * (1.0 / 12.0)


def fields(middle, edge, height):
    lane = lax.broadcasted_iota(jnp.int32, (height, LANES), 1)
    near = [o for o in range(-HALO, HALO + 1) if o]
    centre = middle(0)
    side = edge(0)
    along_rows = {o: middle(o) for o in near}
    slope_r = first(along_rows)
    slope_r_side = first({o: edge(o) for o in (-2, -1, 1, 2)})
    along_cols = {o: shifted(centre, side, lane, o) for o in near}
    slope_c = first(along_cols)
    curve_rc = first({o: shifted(slope_r, slope_r_side, lane, o) for o in (-2, -1, 1, 2)})
    return slope_r, slope_c, second(along_rows, centre), curve_rc, second(along_cols, centre)


def compute_kernel(blocks, where_ref, ratio_ref, pot_ref, win_ref, conv_ref, shear_ref, rot_ref, disp_ref, edges):
    height = conv_ref.shape[0]
    rows = pot_ref.shape[1]
    step = pl.program_id(0)
    beta_near, beta_one, beta_two = ratio_ref[0], ratio_ref[1], ratio_ref[2]
    lane = lax.broadcasted_iota(jnp.int32, (rows, LANES), 1)

    def body(t, carry):
        b = step * TILE + t

        def columns(s):
            return pl.ds(pl.multiple_of(s * LANES, LANES), LANES)

        here = columns(b)
        left = pot_ref[0, :, columns(jnp.where(b == 0, blocks - 1, b - 1))]
        right = pot_ref[0, :, columns(jnp.where(b == blocks - 1, 0, b + 1))]
        edges[0] = edge_of(left, right, lane)
        window = where_ref[b]
        edges[1] = pltpu.roll(win_ref[where_ref[blocks + b]], where_ref[2 * blocks + b], 1)
        near_r, near_c, near_rr, near_rc, near_cc = fields(
            lambda o: pot_ref[0, HALO + o : HALO + o + height, here],
            lambda o: edges[0, HALO + o : HALO + o + height],
            height,
        )
        far_r, far_c, far_rr, far_rc, far_cc = fields(
            lambda o: win_ref[window, HALO + o : HALO + o + height],
            lambda o: edges[1, HALO + o : HALO + o + height],
            height,
        )
        inner_rr = 1.0 - beta_near * near_rr
        inner_rc = -beta_near * near_rc
        inner_cc = 1.0 - beta_near * near_cc
        chain_rr = far_rr * inner_rr + far_rc * inner_rc
        chain_rc = far_rr * inner_rc + far_rc * inner_cc
        chain_cr = far_rc * inner_rr + far_cc * inner_rc
        chain_cc = far_rc * inner_rc + far_cc * inner_cc
        total_rr = 1.0 - beta_one * near_rr - beta_two * chain_rr
        total_rc = -beta_one * near_rc - beta_two * chain_rc
        total_cr = -beta_one * near_rc - beta_two * chain_cr
        total_cc = 1.0 - beta_one * near_cc - beta_two * chain_cc
        there = columns(t)
        conv_ref[:, there] = 1.0 - 0.5 * (total_rr + total_cc)
        shear_ref[0, :, there] = 0.5 * (total_rr - total_cc)
        shear_ref[1, :, there] = -0.5 * (total_rc + total_cr)
        rot_ref[:, there] = 0.5 * (total_rc - total_cr)
        disp_ref[0, :, there] = beta_one * near_r + beta_two * far_r
        disp_ref[1, :, there] = beta_one * near_c + beta_two * far_c
        return carry

    lax.fori_loop(0, TILE, body, 0, unroll=2)


def per_device(potentials, ratios, row_offset, col_offset):
    devices = lax.axis_size("row")
    height, columns = potentials.shape[1:]
    blocks = columns // LANES
    stride = devices // RB
    cap = min(blocks, blocks // RB + SPARE)
    edge_windows = -(-cap // PER_EDGE)
    group = cap + edge_windows
    rows = height + 2 * HALO
    every = jnp.arange(blocks, dtype=jnp.int32)

    counts = jnp.sum(row_offset[:, None] == jnp.arange(RB, dtype=jnp.int32)[None, :], axis=0)
    fullest = jnp.max(counts)
    other = row_offset
    for _ in range(1, lax.axis_size("cosmo")):
        other = passed_along(other, "cosmo", 1)
        theirs = jnp.sum(other[:, None] == jnp.arange(RB, dtype=jnp.int32)[None, :], axis=0)
        fullest = jnp.maximum(fullest, jnp.max(theirs))
    fits = fullest <= cap

    rank = jnp.sum((row_offset[:, None] == row_offset[None, :]) & (every[None, :] < every[:, None]), axis=1)
    slot = jnp.where(fits, row_offset * cap + rank.astype(jnp.int32), every)
    source = (every + col_offset) % blocks
    is_slot = slot[None, :] == jnp.arange(RB * cap, dtype=jnp.int32)[:, None]
    sources = jnp.sum(jnp.where(is_slot, source[None, :], 0), axis=1).astype(jnp.int32)
    chunk, spot = slot // cap, slot % cap
    where = jnp.concatenate([
        chunk * group + spot,
        chunk * group + cap + spot // PER_EDGE,
        LANES - HALO - 2 * HALO * (spot % PER_EDGE),
    ]).astype(jnp.int32)

    above = passed_along(potentials[:, height - HALO :], "row", 1)
    below = passed_along(potentials[:, :HALO], "row", devices - 1)
    padded = jnp.concatenate([above, potentials, below], axis=1)

    packed = pl.pallas_call(
        functools.partial(pack_kernel, cap, blocks),
        out_shape=jax.ShapeDtypeStruct((RB, group, rows, LANES), jnp.float32),
        grid_spec=pltpu.PrefetchScalarGridSpec(
            num_scalar_prefetch=1,
            grid=(RB,),
            in_specs=[pl.BlockSpec((1, rows, columns), lambda g, _: (1, 0, 0))],
            out_specs=pl.BlockSpec((1, group, rows, LANES), lambda g, _: (g, 0, 0, 0)),
        ),
    )(sources, padded)

    def direct(packed):
        return pl.pallas_call(
            functools.partial(exchange_kernel, stride, devices),
            out_shape=jax.ShapeDtypeStruct(packed.shape, packed.dtype),
            in_specs=[pl.BlockSpec(memory_space=pltpu.VMEM)],
            out_specs=pl.BlockSpec(memory_space=pltpu.VMEM),
            scratch_shapes=[
                pltpu.SemaphoreType.DMA((RB,)),
                pltpu.SemaphoreType.DMA((RB,)),
                pltpu.SemaphoreType.DMA,
            ],
            compiler_params=pltpu.CompilerParams(collective_id=0, has_side_effects=True),
        )(packed)

    def by_bits(packed):
        offsets = jnp.sum(jnp.where(is_slot, row_offset[None, :], 0), axis=1).astype(jnp.int32).reshape(RB, cap)
        of_edges = jnp.pad(offsets, ((0, 0), (0, edge_windows * PER_EDGE - cap)))
        of_edges = jnp.repeat(of_edges.reshape(RB, edge_windows, PER_EDGE), 2 * HALO, axis=2)
        lanes = jnp.concatenate([jnp.broadcast_to(offsets[:, :, None], (RB, cap, LANES)), of_edges], axis=1)
        for bit in range(BITS):
            arrived = passed_along(packed, "row", devices - stride * 2**bit)
            picked = lanes // 2**bit % 2 == 1
            packed = jnp.where(picked[:, :, None, :], arrived, packed)
        return packed

    windows = lax.cond(fits, direct, by_bits, packed).reshape(RB * group, rows, LANES)

    wide = TILE * LANES
    return pl.pallas_call(
        functools.partial(compute_kernel, blocks),
        out_shape=(
            jax.ShapeDtypeStruct((height, columns), jnp.float32),
            jax.ShapeDtypeStruct((2, height, columns), jnp.float32),
            jax.ShapeDtypeStruct((height, columns), jnp.float32),
            jax.ShapeDtypeStruct((2, height, columns), jnp.float32),
        ),
        grid_spec=pltpu.PrefetchScalarGridSpec(
            num_scalar_prefetch=2,
            grid=(blocks // TILE,),
            in_specs=[
                pl.BlockSpec((1, rows, columns), lambda g, *_: (0, 0, 0)),
                pl.BlockSpec((RB * group, rows, LANES), lambda g, *_: (0, 0, 0)),
            ],
            out_specs=(
                pl.BlockSpec((height, wide), lambda g, *_: (0, g)),
                pl.BlockSpec((2, height, wide), lambda g, *_: (0, 0, g)),
                pl.BlockSpec((height, wide), lambda g, *_: (0, g)),
                pl.BlockSpec((2, height, wide), lambda g, *_: (0, 0, g)),
            ),
            scratch_shapes=[pltpu.VMEM((2, rows, LANES), jnp.float32)],
        ),
    )(where, ratios, padded, windows)


def solution(mesh):
    return jax.shard_map(
        per_device,
        mesh=mesh,
        in_specs=(P("cosmo", "row", None), P("cosmo"), P("cosmo"), P("cosmo")),
        out_specs=(
            P(("cosmo", "row"), None),
            P(None, ("cosmo", "row"), None),
            P(("cosmo", "row"), None),
            P(None, ("cosmo", "row"), None),
        ),
        check_vma=False,
    )
```

```python
import functools

import jax
import jax.numpy as jnp
from jax import lax
from jax.experimental import pallas as pl
from jax.experimental.pallas import tpu as pltpu
from jax.sharding import PartitionSpec as P

RB = 8
BITS = 3
LANES = 128
HALO = 4
PER_EDGE = LANES // (2 * HALO)
SPARES = (6, 8, 10, 12, 16)
TILE = 16


def passed_along(x, axis, by):
    size = lax.axis_size(axis)
    return lax.ppermute(x, axis, [(i, (i + by) % size) for i in range(size)])


def edge_of(left, right, lane):
    return jnp.where(lane < LANES // 2, right, left)


def pack_kernel(cap, edge_windows, blocks, src_ref, pot_ref, out_ref):
    group = pl.program_id(0)
    rows = pot_ref.shape[1]
    lane = lax.broadcasted_iota(jnp.int32, (rows, LANES), 1)

    def columns(s):
        return pl.ds(pl.multiple_of(s * LANES, LANES), LANES)

    packed = None
    for j in range(cap):
        s = src_ref[group * cap + j]
        left = pot_ref[0, :, columns(jnp.where(s == 0, blocks - 1, s - 1))]
        right = pot_ref[0, :, columns(jnp.where(s == blocks - 1, 0, s + 1))]
        for q in range(rows // HALO):
            out_ref[0, q, edge_windows + j] = pot_ref[0, HALO * q : HALO * (q + 1), columns(s)]
        spot = j % PER_EDGE
        edge = pltpu.roll(edge_of(left, right, lane), HALO + 2 * HALO * spot, 1)
        packed = edge if spot == 0 else jnp.where(lane >= 2 * HALO * spot, edge, packed)
        if spot == PER_EDGE - 1 or j == cap - 1:
            for q in range(rows // HALO):
                out_ref[0, q, j // PER_EDGE] = packed[HALO * q : HALO * (q + 1)]


def exchange_kernel(
    stride, devices, used, buf_ref, top_ref, bottom_ref, out_ref, above_ref, below_ref,
    send_sem, recv_sem, up_send, up_recv, down_send, down_recv, own_sem,
):
    me = lax.axis_index("row")
    quads = buf_ref.shape[1]
    part = pl.ds(0, used)
    after, before = lax.rem(me + 1, devices), lax.rem(me + devices - 1, devices)
    peers = [lax.rem(me + stride * k, devices) for k in range(1, RB)] + [after, before]
    barrier = pltpu.get_barrier_semaphore()
    for peer in peers:
        pl.semaphore_signal(barrier, inc=1, device_id={"row": peer}, device_id_type=pl.DeviceIdType.MESH)
    pl.semaphore_wait(barrier, len(peers))

    def sent(src, dst, send, recv, to):
        copy = pltpu.make_async_remote_copy(
            src_ref=src, dst_ref=dst, send_sem=send, recv_sem=recv,
            device_id={"row": to}, device_id_type=pl.DeviceIdType.MESH,
        )
        copy.start()
        return copy

    order = sorted(range(1, RB), key=lambda k: abs(k - RB // 2))
    copies = {
        k: sent(
            buf_ref.at[k, :, part], out_ref.at[k, pl.ds(1, quads), part], send_sem.at[k], recv_sem.at[k],
            lax.rem(me + devices - stride * k, devices),
        )
        for k in order
    }
    own = pltpu.make_async_copy(buf_ref.at[0, :, part], out_ref.at[0, pl.ds(1, quads), part], own_sem)
    own.start()
    rims = [
        sent(bottom_ref, above_ref, up_send.at[RB], up_recv.at[RB], after),
        sent(top_ref, below_ref, down_send.at[RB], down_recv.at[RB], before),
        sent(buf_ref.at[0, quads - 1, part], out_ref.at[0, 0, part], up_send.at[0], up_recv.at[0], after),
        sent(buf_ref.at[0, 0, part], out_ref.at[0, quads + 1, part], down_send.at[0], down_recv.at[0], before),
    ]
    for k in order:
        copies[k].wait_recv()
        rims.append(sent(out_ref.at[k, quads, part], out_ref.at[k, 0, part], up_send.at[k], up_recv.at[k], after))
        rims.append(sent(out_ref.at[k, 1, part], out_ref.at[k, quads + 1, part], down_send.at[k], down_recv.at[k], before))
    own.wait()
    for k in order:
        copies[k].wait_send()
    for copy in rims:
        copy.wait()


def shifted(middle, edge, lane, by):
    if by > 0:
        return pltpu.roll(jnp.where(lane < by, edge, middle), LANES - by, 1)
    return pltpu.roll(jnp.where(lane >= LANES + by, edge, middle), -by, 1)


def second(x, total):
    return (
        (x[4] + x[-4]) - 16.0 * (x[3] + x[-3]) + 64.0 * (x[2] + x[-2])
        + 16.0 * (x[1] + x[-1]) - 130.0 * total
    ) * (1.0 / 144.0)


def first(x):
    return (8.0 * (x[1] - x[-1]) - (x[2] - x[-2])) * (1.0 / 12.0)


def fields(middle, edge, height):
    lane = lax.broadcasted_iota(jnp.int32, (height, LANES), 1)
    near = [o for o in range(-HALO, HALO + 1) if o]
    centre = middle(0)
    side = edge(0)
    along_rows = {o: middle(o) for o in near}
    slope_r = first(along_rows)
    slope_r_side = first({o: edge(o) for o in (-2, -1, 1, 2)})
    along_cols = {o: shifted(centre, side, lane, o) for o in near}
    slope_c = first(along_cols)
    curve_rc = first({o: shifted(slope_r, slope_r_side, lane, o) for o in (-2, -1, 1, 2)})
    return slope_r, slope_c, second(along_rows, centre), curve_rc, second(along_cols, centre)


def compute_kernel(
    blocks, where_ref, ratio_ref, pot_ref, above_ref, below_ref, win_ref,
    conv_ref, shear_ref, rot_ref, disp_ref, views,
):
    height = conv_ref.shape[0]
    rows = height + 2 * HALO
    step = pl.program_id(0)
    beta_near, beta_one, beta_two = ratio_ref[0], ratio_ref[1], ratio_ref[2]

    def body(t, carry):
        b = step * TILE + t

        def columns(s):
            return pl.ds(pl.multiple_of(s * LANES, LANES), LANES)

        here = columns(b)
        left = columns(jnp.where(b == 0, blocks - 1, b - 1))
        right = columns(jnp.where(b == blocks - 1, 0, b + 1))
        view = views.at[lax.rem(t, 2)]
        for rim, ref in ((slice(0, HALO), above_ref), (slice(HALO, HALO + height), pot_ref.at[0]), (slice(HALO + height, rows), below_ref)):
            lane = lax.broadcasted_iota(jnp.int32, (ref.shape[0], LANES), 1)
            view[0, rim] = ref[:, here]
            view[1, rim] = edge_of(ref[:, left], ref[:, right], lane)
        chunk, window, edge = where_ref[b], where_ref[blocks + b], where_ref[2 * blocks + b]
        turn = where_ref[3 * blocks + b]
        for q in range(rows // HALO):
            view[2, HALO * q : HALO * (q + 1)] = win_ref[chunk, q, window]
            view[3, HALO * q : HALO * (q + 1)] = win_ref[chunk, q, edge]
        view[3] = pltpu.roll(view[3], turn, 1)

        def rows_of(n):
            return lambda o: view[n, HALO + o : HALO + o + height]

        near_r, near_c, near_rr, near_rc, near_cc = fields(rows_of(0), rows_of(1), height)
        far_r, far_c, far_rr, far_rc, far_cc = fields(rows_of(2), rows_of(3), height)
        inner_rr = 1.0 - beta_near * near_rr
        inner_rc = -beta_near * near_rc
        inner_cc = 1.0 - beta_near * near_cc
        chain_rr = far_rr * inner_rr + far_rc * inner_rc
        chain_rc = far_rr * inner_rc + far_rc * inner_cc
        chain_cr = far_rc * inner_rr + far_cc * inner_rc
        chain_cc = far_rc * inner_rc + far_cc * inner_cc
        total_rr = 1.0 - beta_one * near_rr - beta_two * chain_rr
        total_rc = -beta_one * near_rc - beta_two * chain_rc
        total_cr = -beta_one * near_rc - beta_two * chain_cr
        total_cc = 1.0 - beta_one * near_cc - beta_two * chain_cc
        there = columns(t)
        conv_ref[:, there] = 1.0 - 0.5 * (total_rr + total_cc)
        shear_ref[0, :, there] = 0.5 * (total_rr - total_cc)
        shear_ref[1, :, there] = -0.5 * (total_rc + total_cr)
        rot_ref[:, there] = 0.5 * (total_rc - total_cr)
        disp_ref[0, :, there] = beta_one * near_r + beta_two * far_r
        disp_ref[1, :, there] = beta_one * near_c + beta_two * far_c
        return carry

    lax.fori_loop(0, TILE, body, 0, unroll=2)


def per_device(potentials, ratios, row_offset, col_offset):
    devices = lax.axis_size("row")
    height, columns = potentials.shape[1:]
    blocks = columns // LANES
    stride = devices // RB
    caps = [min(blocks, blocks // RB + spare) for spare in SPARES]
    cap = caps[-1]
    edge_windows = -(-cap // PER_EDGE)
    group = cap + edge_windows
    quads = height // HALO
    every = jnp.arange(blocks, dtype=jnp.int32)

    rank = None
    fullest = 0
    other = row_offset
    for turn in range(lax.axis_size("cosmo")):
        if turn:
            other = passed_along(other, "cosmo", 1)
        ranks = jnp.sum((other[:, None] == other[None, :]) & (every[None, :] < every[:, None]), axis=1, dtype=jnp.int32)
        fullest = jnp.maximum(fullest, jnp.max(ranks) + 1)
        rank = ranks if rank is None else rank
    level = sum((fullest > c).astype(jnp.int32) for c in caps)

    slot = jnp.where(fullest <= cap, row_offset * cap + rank, every)
    source = (every + col_offset) % blocks
    is_slot = slot[None, :] == jnp.arange(RB * cap, dtype=jnp.int32)[:, None]
    sources = jnp.sum(jnp.where(is_slot, source[None, :], 0), axis=1, dtype=jnp.int32)
    spot = slot % cap
    where = jnp.concatenate([
        slot // cap,
        edge_windows + spot,
        spot // PER_EDGE,
        LANES - HALO - 2 * HALO * (spot % PER_EDGE),
    ]).astype(jnp.int32)

    packed = pl.pallas_call(
        functools.partial(pack_kernel, cap, edge_windows, blocks),
        out_shape=jax.ShapeDtypeStruct((RB, quads, group, HALO, LANES), jnp.float32),
        grid_spec=pltpu.PrefetchScalarGridSpec(
            num_scalar_prefetch=1,
            grid=(RB,),
            in_specs=[pl.BlockSpec((1, height, columns), lambda g, _: (1, 0, 0))],
            out_specs=pl.BlockSpec((1, quads, group, HALO, LANES), lambda g, _: (g, 0, 0, 0, 0)),
        ),
    )(sources, potentials)
    top, bottom = potentials[0, :HALO], potentials[0, height - HALO :]
    out_shape = (RB, quads + 2, group, HALO, LANES)

    def direct(n, packed, top, bottom):
        vmem = pl.BlockSpec(memory_space=pltpu.VMEM)
        return pl.pallas_call(
            functools.partial(exchange_kernel, stride, devices, edge_windows + caps[n]),
            out_shape=tuple(jax.ShapeDtypeStruct(x, jnp.float32) for x in (out_shape, top.shape, top.shape)),
            in_specs=[vmem] * 3,
            out_specs=(vmem,) * 3,
            scratch_shapes=[pltpu.SemaphoreType.DMA((RB,))] * 2
            + [pltpu.SemaphoreType.DMA((RB + 1,))] * 4
            + [pltpu.SemaphoreType.DMA],
            compiler_params=pltpu.CompilerParams(collective_id=n, has_side_effects=True),
        )(packed, top, bottom)

    def by_bits(packed, top, bottom):
        offsets = jnp.sum(jnp.where(is_slot, row_offset[None, :], 0), axis=1, dtype=jnp.int32).reshape(RB, cap)
        of_edges = jnp.pad(offsets, ((0, 0), (0, edge_windows * PER_EDGE - cap)))
        of_edges = jnp.repeat(of_edges.reshape(RB, edge_windows, PER_EDGE), 2 * HALO, axis=2)
        lanes = jnp.concatenate([of_edges, jnp.broadcast_to(offsets[:, :, None], (RB, cap, LANES))], axis=1)
        for bit in range(BITS):
            arrived = passed_along(packed, "row", devices - stride * 2**bit)
            picked = lanes // 2**bit % 2 == 1
            packed = jnp.where(picked[:, None, :, None, :], arrived, packed)
        over = passed_along(packed[:, quads - 1 :], "row", 1)
        under = passed_along(packed[:, :1], "row", devices - 1)
        return (
            jnp.concatenate([over, packed, under], axis=1),
            passed_along(bottom, "row", 1),
            passed_along(top, "row", devices - 1),
        )

    branches = [functools.partial(direct, n) for n in range(len(caps))] + [by_bits]
    windows, above, below = lax.switch(level, branches, packed, top, bottom)

    wide = TILE * LANES
    return pl.pallas_call(
        functools.partial(compute_kernel, blocks),
        out_shape=(
            jax.ShapeDtypeStruct((height, columns), jnp.float32),
            jax.ShapeDtypeStruct((2, height, columns), jnp.float32),
            jax.ShapeDtypeStruct((height, columns), jnp.float32),
            jax.ShapeDtypeStruct((2, height, columns), jnp.float32),
        ),
        grid_spec=pltpu.PrefetchScalarGridSpec(
            num_scalar_prefetch=2,
            grid=(blocks // TILE,),
            in_specs=[
                pl.BlockSpec((1, height, columns), lambda g, *_: (0, 0, 0)),
                pl.BlockSpec((HALO, columns), lambda g, *_: (0, 0)),
                pl.BlockSpec((HALO, columns), lambda g, *_: (0, 0)),
                pl.BlockSpec(out_shape, lambda g, *_: (0, 0, 0, 0, 0)),
            ],
            out_specs=(
                pl.BlockSpec((height, wide), lambda g, *_: (0, g)),
                pl.BlockSpec((2, height, wide), lambda g, *_: (0, 0, g)),
                pl.BlockSpec((height, wide), lambda g, *_: (0, g)),
                pl.BlockSpec((2, height, wide), lambda g, *_: (0, 0, g)),
            ),
            scratch_shapes=[pltpu.VMEM((2, 4, height + 2 * HALO, LANES), jnp.float32)],
        ),
    )(where, ratios, potentials, above, below, windows)


def solution(mesh):
    return jax.shard_map(
        per_device,
        mesh=mesh,
        in_specs=(P("cosmo", "row", None), P("cosmo"), P("cosmo"), P("cosmo")),
        out_specs=(
            P(("cosmo", "row"), None),
            P(None, ("cosmo", "row"), None),
            P(("cosmo", "row"), None),
            P(None, ("cosmo", "row"), None),
        ),
        check_vma=False,
    )
```
